32 devices in a mesh: rows: 8 (over z, y), cols: 4 (over x, core).
Axes of the slice: x: 2, y: 2, z: 4, core: 2. Of those that a mesh axis runs over, the one named last changes fastest.
Arguments:
- projector_matrix: float32 [8192, 4096], P('rows', 'cols'), may hold values from -0.0625 to 0.0625
- start_state: float32 [128, 4096], P(None, 'cols'), may hold values from -6 to 6
- decay_rate: float32 [4096], P('cols'), may hold values from 0.05 to 0.95
- escape_heat_factor: float32 [8192], P('rows'), may hold values from 0.1 to 1
- tile_block: int32 [64], P('rows'), may hold values from 0 to 63, as said below
- block_owner: int32 [64], replicated, may hold values from 0 to 7, as said below
- owner_power: float32 [4, 128, 64], P(None, None, 'rows'), may hold values from 0.2 to 5
Outputs:
- final_state: float32 [128, 4096], P(None, 'cols')
- node_temps: float32 [128, 8192], P('cols', 'rows')
- block_history: float32 [4, 128, 64], P(None, 'cols', 'rows')
The draws below stay inside these ranges and needn't reach their ends.
Inputs may be any that keep to these rules, and one draw needn't show every extreme that they name: `block_owner`: every rows index owns exactly 8 blocks. `tile_block`: each block is named by exactly one tile.
All inputs are finite; a program needn't handle non-finite values.
Results may differ from the reference program's by a relative error of at most 0.0001.
Values sent between devices are 32-bit elements; how exact they have to be, the bound alone decides.
No kernel may reach another device: no remote copies, remote signals or barrier semaphores. Data moves between devices by JAX's collectives and lax.ppermute only.
A program may use at most 64 MiB of HBM per device.

```python
import math
import jax
import jax.numpy as jnp
from jax import lax

Q = 4096
HEAT_SCENES = 128
STEPS = 4
PATCH_POINTS = 128
MESH_POINTS = 8192
PATCH_TOTAL = 64
BLOCKS = 64
BLK_DEV = 8
N_ROWS = 8


def joint_floorplan(key):
    owner_key = jax.random.fold_in(key, 11)
    offset_key = jax.random.fold_in(key, 23)
    slot_key = jax.random.fold_in(key, 37)
    shuffled = jax.random.permutation(owner_key, jnp.arange(BLOCKS, dtype=jnp.int32))
    owners = (shuffled // BLK_DEV).astype(jnp.int32)
    grouped = jnp.argsort(owners, stable=True).astype(jnp.int32)
    half_rows = N_ROWS // 2
    offsets = jax.random.randint(offset_key, (BLK_DEV,), 0, half_rows, dtype=jnp.int32) * 2
    slots_all = jnp.arange(BLK_DEV, dtype=jnp.int32)
    offsets = (offsets + jnp.where(slots_all == 0, 1, 0)).astype(jnp.int32)
    tiles = jnp.arange(PATCH_TOTAL, dtype=jnp.int32)
    holder = tiles // BLK_DEV
    slot = tiles % BLK_DEV
    target = (3 * holder + offsets[slot]) % N_ROWS
    rotate = jax.random.randint(slot_key, (N_ROWS,), 0, BLK_DEV, dtype=jnp.int32)
    place = (slot + rotate[target]) % BLK_DEV
    picked = grouped[target * BLK_DEV + place]
    return (owners, picked.astype(jnp.int32))


def draw_block_owner(key, part):
    owners, picked = joint_floorplan(key)
    return owners


def draw_tile_block(key, part):
    owners, picked = joint_floorplan(key)
    return picked


def shard_levels(rng, dims, split, least, high):
    factor_of, own = 1.0, jax.random.fold_in(rng, 6)
    for dim, shards_of in split:
        steps = jnp.exp(jax.random.uniform(jax.random.fold_in(own, dim), (shards_of,), jnp.float32, least / len(split), high / len(split)))
        factor_of = factor_of * jnp.repeat(steps, dims[dim] // shards_of).reshape([-1 if axis == dim else 1 for axis in range(len(dims))])
    return factor_of


def gaussian(own_key, shape, width, most, split=(), kind=jnp.bfloat16):
    drawn = jax.random.normal(own_key, shape, jnp.float32) * width
    if len(split) > 0:
        drawn = shard_levels(own_key, shape, split, -0.22, 0.18) * drawn
    return jnp.clip(drawn, min=-most, max=most).astype(kind)


def setup_inputs(seed: int = 0) -> dict:
    splits = jax.random.split(jax.random.key(seed), 8)
    projector_matrix = gaussian(splits[0], (MESH_POINTS, Q), MESH_POINTS ** -0.5, 0.0625, ((0, 8), (1, 4)), jnp.float32)
    start_state = gaussian(splits[1], (HEAT_SCENES, Q), 1.0, 6.0, ((1, 4),), jnp.float32)
    decay_rate = jnp.clip(jnp.exp(math.log(0.95) - 2.944439 * jax.random.uniform(splits[2], (Q,), jnp.float32) ** shard_levels(splits[2], (Q,), ((0, 4),), -0.2, 0.2)), 0.05, 0.95)
    escape_heat_factor = jnp.clip(jnp.exp(math.log(1.0) - 2.3025851 * jax.random.uniform(splits[3], (MESH_POINTS,), jnp.float32) ** shard_levels(splits[3], (MESH_POINTS,), ((0, 8),), -0.2, 0.2)), 0.1, 1.0)
    tile_block = draw_tile_block(jax.random.fold_in(splits[7], 71), 0)
    block_owner = draw_block_owner(jax.random.fold_in(splits[7], 71), 0)
    owner_power = jnp.clip(jnp.exp(math.log(5.0) - 3.218876 * jax.random.uniform(splits[6], (STEPS, HEAT_SCENES, BLOCKS), jnp.float32) ** shard_levels(splits[6], (STEPS, HEAT_SCENES, BLOCKS), ((2, 8),), -0.2, 0.2)), 0.2, 5.0)
    return {"projector_matrix": projector_matrix, "start_state": start_state, "decay_rate": decay_rate, "escape_heat_factor": escape_heat_factor, "tile_block": tile_block, "block_owner": block_owner, "owner_power": owner_power}


escape_heat_derivative = 2.0
dominant_spectral_direction = lax.Precision.HIGHEST


def floor_positions(block_owner, per_owner):
    indices = jnp.arange(block_owner.shape[0], dtype=jnp.int32)
    same_owner = (block_owner[:, None] == block_owner[None, :]) & (indices[None, :] < indices[:, None])
    return block_owner * per_owner + jnp.sum(same_owner.astype(jnp.int32), axis=1)


def reference(projector_matrix, start_state, decay_rate, escape_heat_factor, tile_block, block_owner, owner_power):
    positions = floor_positions(block_owner, BLK_DEV)
    tile_position = positions[tile_block]
    columns = jnp.arange(BLOCKS, dtype=jnp.int32)
    tile_onehot = (tile_position[:, None] == columns[None, :]).astype(jnp.float32)
    compact_vector = start_state
    march_history = []
    point_heat_level = jnp.zeros((HEAT_SCENES, MESH_POINTS), jnp.float32)
    for step_index in range(STEPS):
        point_heat_level = jnp.einsum("ec,wc->ew", compact_vector, projector_matrix, precision=dominant_spectral_direction)
        patch_mean_level = jnp.sum(point_heat_level.reshape(HEAT_SCENES, PATCH_TOTAL, PATCH_POINTS), axis=2) * (1.0 / PATCH_POINTS)
        march_history.append(jnp.dot(patch_mean_level, tile_onehot, precision=dominant_spectral_direction))
        heating_at_patches = jnp.einsum("sb,tb->st", owner_power[step_index], tile_onehot, precision=dominant_spectral_direction)
        heating_at_points = jnp.repeat(heating_at_patches, PATCH_POINTS, axis=1) + escape_heat_factor[None, :] * (1.0 + jnp.tanh(escape_heat_derivative * point_heat_level))
        driven = jnp.dot(heating_at_points, projector_matrix, precision=dominant_spectral_direction)
        compact_vector = decay_rate * compact_vector + (1.0 - decay_rate) * driven
    return compact_vector, point_heat_level, jnp.stack(march_history)
```

```python
import jax
import jax.numpy as jnp
from jax import lax
from jax.sharding import PartitionSpec as P

STEPS = 4
PATCH_POINTS = 128
GROUPS = 1
DIRECT_MAX = 8


exact = lax.Precision.HIGHEST
three_pass = lax.Precision.HIGH


def floor_positions(block_owner, per_owner):
    indices = jnp.arange(block_owner.shape[0], dtype=jnp.int32)
    same_owner = (block_owner[:, None] == block_owner[None, :]) & (
        indices[None, :] < indices[:, None]
    )
    return block_owner * per_owner + jnp.sum(same_owner.astype(jnp.int32), axis=1)


def shift(x, axis, k):
    n = lax.axis_size(axis)
    return lax.ppermute(x, axis, [(i, (i + k) % n) for i in range(n)])


def swap(x, axis, bit):
    n = lax.axis_size(axis)
    return lax.ppermute(x, axis, [(i, i ^ bit) for i in range(n)])


def rows_gather(x):
    n = lax.axis_size("rows")
    if n > DIRECT_MAX:
        return lax.all_gather(x, "rows", axis=0, tiled=True)
    parts = [x] + [shift(x, "rows", k) for k in range(1, n)]
    ordered = jnp.concatenate(parts[::-1] + parts[::-1][:-1], axis=0)
    start = (n - 1 - lax.axis_index("rows")) * x.shape[0]
    return lax.dynamic_slice_in_dim(ordered, start, n * x.shape[0], 0)


def rows_scatter_sum(x):
    n = lax.axis_size("rows")
    if n > DIRECT_MAX:
        return lax.psum_scatter(x, "rows", scatter_dimension=0, tiled=True)
    r = lax.axis_index("rows")
    p = x.shape[0] // n
    got = []
    for k in range(n):
        piece = lax.dynamic_slice_in_dim(x, ((r + k) % n) * p, p, 0)
        got.append(piece if k == 0 else shift(piece, "rows", k))
    while len(got) > 1:
        got = [a + b for a, b in zip(got[::2], got[1::2])]
    return got[0]


def shards(
    projector_matrix,
    start_state,
    decay_rate,
    escape_heat_factor,
    tile_block,
    block_owner,
    owner_power,
):
    nodes, states = projector_matrix.shape
    scen = start_state.shape[0]
    n_rows, n_cols = lax.axis_size("rows"), lax.axis_size("cols")
    r, c = lax.axis_index("rows"), lax.axis_index("cols")
    pair, half = c % 2, c // 2
    halves = n_cols // 2
    share = scen // n_cols
    groups = GROUPS if scen // (n_rows * GROUPS) >= 8 else 1
    m = share // groups
    rows_g = scen // groups
    piece = rows_g // n_rows
    tiles = tile_block.shape[0]

    power = owner_power.reshape(STEPS, halves, 2, share, tiles)
    power = lax.dynamic_index_in_dim(power, pair, 2, keepdims=False)
    power = power.reshape(STEPS * halves * share, tiles).T
    power = rows_gather(power)

    positions = floor_positions(block_owner, tiles)
    tile_position = jnp.take(positions, tile_block)
    columns = jnp.arange(block_owner.shape[0], dtype=jnp.int32)
    tile_onehot = (tile_position[:, None] == columns[None, :]).astype(jnp.float32)
    heat = jnp.dot(tile_onehot, power, precision=exact)
    heat = heat.reshape(tiles, STEPS, halves, groups, m)

    start = start_state.reshape(n_cols, groups, m, states)
    state = [start[:, g].reshape(rows_g, states) for g in range(groups)]
    mine = [lax.dynamic_slice_in_dim(s, r * piece, piece, 0) for s in state]
    keep = decay_rate[None, :]
    own_temp = [None] * groups
    history = []
    for step in range(STEPS):
        level = []
        for g in range(groups):
            part = jnp.einsum("ec,wc->ew", state[g], projector_matrix, precision=three_pass)
            part = part.reshape(halves, 2, m, nodes)
            away = lax.dynamic_index_in_dim(part, 1 - pair, 1, keepdims=False)
            stay = lax.dynamic_index_in_dim(part, pair, 1, keepdims=False)
            temp = stay + swap(away, "cols", 1)
            if n_cols == 4:
                temp = temp + swap(temp, "cols", 2)
            else:
                others = [(h, 2 * h) for h in range(1, halves)]
                temp = sum([temp] + [shift(temp, "cols", k) for _, k in others])
            own = lax.dynamic_index_in_dim(temp, half, 0, keepdims=False)
            own_temp[g] = own
            level.append(
                jnp.sum(own.reshape(m, tiles, PATCH_POINTS), axis=2) * (1.0 / PATCH_POINTS)
            )
            at_tiles = jnp.transpose(heat[:, step, :, g], (1, 2, 0))
            spread = jnp.broadcast_to(
                at_tiles[..., None], (halves, m, tiles, PATCH_POINTS)
            ).reshape(halves, m, nodes)
            heating = spread + escape_heat_factor * (1.0 + jnp.tanh(2.0 * temp))
            other = swap(heating, "cols", 1)
            first = jnp.where(pair == 0, heating, other)
            second = jnp.where(pair == 0, other, heating)
            full = jnp.stack([first, second], axis=1).reshape(rows_g, nodes)
            driven = jnp.dot(full, projector_matrix, precision=three_pass)
            driven = rows_scatter_sum(driven)
            mine[g] = keep * mine[g] + (1.0 - keep) * driven
            state[g] = rows_gather(mine[g])
        history.append(jnp.stack(level, 0).reshape(share, tiles))
    final = jnp.stack([s.reshape(n_cols, m, states) for s in state], 1).reshape(scen, states)
    temps = jnp.stack(own_temp, 0).reshape(share, nodes)
    levels = jnp.stack(history).reshape(STEPS * share, tiles)
    blocks = lax.dot_general(
        tile_onehot, levels, (((0,), (1,)), ((), ())), precision=exact
    )
    blocks = rows_scatter_sum(blocks)
    blocks = jnp.transpose(blocks.reshape(tiles, STEPS, share), (1, 2, 0))
    return (final, temps, blocks)


def solution(mesh):
    placed = (
        P("rows", "cols"),
        P(None, "cols"),
        P("cols"),
        P("rows"),
        P("rows"),
        P(),
        P(None, None, "rows"),
    )
    return jax.shard_map(
        shards,
        mesh=mesh,
        in_specs=placed,
        out_specs=(P(None, "cols"), P("cols", "rows"), P(None, "cols", "rows")),
        check_vma=False,
    )
```

```python
import jax
import jax.numpy as jnp
from jax import lax
from jax.sharding import PartitionSpec as P

STEPS = 4
PATCH_POINTS = 128
DIRECT_MAX = 4
RELAY = False


exact = lax.Precision.HIGHEST


def floor_positions(block_owner, per_owner):
    indices = jnp.arange(block_owner.shape[0], dtype=jnp.int32)
    same_owner = (block_owner[:, None] == block_owner[None, :]) & (
        indices[None, :] < indices[:, None]
    )
    return block_owner * per_owner + jnp.sum(same_owner.astype(jnp.int32), axis=1)


def swap(x, axis, bit):
    n = lax.axis_size(axis)
    return lax.ppermute(x, axis, [(i, i ^ bit) for i in range(n)])


def outer_shift(x, k, inner):
    n = lax.axis_size("rows")
    return lax.ppermute(x, "rows", [(i, (i + k * inner) % n) for i in range(n)])


def halves_of(x):
    high = lax.reduce_precision(x, 8, 7)
    return high.astype(jnp.bfloat16), (x - high).astype(jnp.bfloat16)


def product(x, basis):
    high, low = halves_of(x)
    both = jnp.concatenate([high, low], 0)
    dims = (((1,), (basis[2],)), ((), ()))
    main = lax.dot_general(both, basis[0], dims, preferred_element_type=jnp.float32)
    rest = lax.dot_general(high, basis[1], dims, preferred_element_type=jnp.float32)
    return main[: x.shape[0]] + (main[x.shape[0] :] + rest)


def shards(
    projector_matrix,
    start_state,
    decay_rate,
    escape_heat_factor,
    tile_block,
    block_owner,
    owner_power,
):
    nodes, states = projector_matrix.shape
    scen = start_state.shape[0]
    n_rows, n_cols = lax.axis_size("rows"), lax.axis_size("cols")
    r, c = lax.axis_index("rows"), lax.axis_index("cols")
    pair, half = c % 2, c // 2
    pairs = n_cols // 2
    share = scen // n_cols
    held = pairs * share
    tiles = tile_block.shape[0]
    inner = 2 if n_rows % 2 == 0 else 1
    outer = n_rows // inner
    direct = outer <= DIRECT_MAX and held % outer == 0 and inner == 2
    if not direct:
        outer, inner = 1, 1
    z, y = r // inner, r % inner
    piece = held // outer

    def relative(x, axis=0):
        size = x.shape[axis] // outer
        got = [
            lax.dynamic_slice_in_dim(x, ((z - j) % outer) * size, size, axis)
            for j in range(outer)
        ]
        return jnp.concatenate(got, axis) if outer > 1 else got[0]

    def of_pair(x, which):
        x = x.reshape((pairs, 2, share) + x.shape[1:])
        x = lax.dynamic_index_in_dim(x, which, 1, keepdims=False)
        return x.reshape((held,) + x.shape[2:])

    basis = [halves_of(b) for b in (projector_matrix, swap(projector_matrix, "cols", 1))]
    keep = jnp.concatenate([decay_rate, swap(decay_rate, "cols", 1)])[None, :]
    state = jnp.concatenate(
        [
            of_pair(start_state, pair),
            swap(of_pair(start_state, 1 - pair), "cols", 1),
        ],
        1,
    )
    state = relative(state)

    power = jnp.moveaxis(owner_power, 0, 1)
    power = relative(of_pair(power, pair))
    power = power.reshape(held * STEPS, tiles).T
    positions = floor_positions(block_owner, tiles)
    tile_position = jnp.take(positions, tile_block)
    columns = jnp.arange(block_owner.shape[0], dtype=jnp.int32)
    tile_onehot = (tile_position[:, None] == columns[None, :]).astype(jnp.float32)
    if direct:
        power = jnp.concatenate([power, swap(power, "rows", 1)], 0)
        power = power.reshape(inner * tiles, outer, piece * STEPS)
        seen = []
        for k in range(outer):
            came = outer_shift(power, k, inner) if k else power
            seen.append(jnp.roll(came, k, axis=1))
        power = jnp.concatenate(seen, 0).reshape(n_rows * tiles, held * STEPS)
        owner = tile_position // tiles
        rel = ((z - owner // inner) % outer) * inner + (y + owner % inner) % inner
        rel = rel * tiles + tile_position % tiles
        pick = (rel[:, None] == columns[None, :]).astype(jnp.float32)
    else:
        power = lax.all_gather(power, "rows", axis=0, tiled=True)
        pick = tile_onehot
    heat = jnp.dot(pick, power, precision=exact).reshape(tiles, held, STEPS)

    mine = state[:piece]
    levels = []
    for step in range(STEPS):
        temp = product(state[:, :states], basis[0] + (1,)) + product(
            state[:, states:], basis[1] + (1,)
        )
        if pairs == 2:
            temp = temp + swap(temp, "cols", 2)
        else:
            temp = sum(
                [temp]
                + [
                    lax.ppermute(temp, "cols", [(i, (i + 2 * h) % n_cols) for i in range(n_cols)])
                    for h in range(1, pairs)
                ]
            )
        levels.append(
            jnp.sum(temp.reshape(held, tiles, PATCH_POINTS), axis=2) * (1.0 / PATCH_POINTS)
        )
        spread = jnp.broadcast_to(
            heat[:, :, step].T[:, :, None], (held, tiles, PATCH_POINTS)
        ).reshape(held, nodes)
        heating = spread + escape_heat_factor * (1.0 + jnp.tanh(2.0 * temp))
        driven = jnp.concatenate([product(heating, b + (0,)) for b in basis], 1)
        last = step == STEPS - 1
        if last:
            def own(x):
                if outer % pairs == 0 and outer > 1:
                    per = outer // pairs
                    x = x.reshape((outer, piece) + x.shape[1:])
                    got = [
                        lax.dynamic_index_in_dim(x, (z - half * per - q) % outer, 0, keepdims=False)
                        for q in range(per)
                    ]
                    return jnp.concatenate(got, 0)
                return lax.dynamic_slice_in_dim(x, half * share, share, 0)

            temps = own(temp)
            level = jnp.stack([own(v) for v in levels]).reshape(STEPS * share, tiles)
            blocks = lax.dot_general(
                tile_onehot, level, (((0,), (1,)), ((), ())), precision=exact
            )
        if direct:
            parts = [driven[j * piece : (j + 1) * piece] for j in range(outer)]
            ride = last and piece == inner * tiles
            if ride:
                hist = relative(blocks)
                parts = [
                    jnp.concatenate([p, hist[j * piece : (j + 1) * piece]], 1)
                    for j, p in enumerate(parts)
                ]
            total = parts[0]
            for j in range(1, outer):
                total = total + outer_shift(parts[j], -j, inner)
            total = total + swap(total, "rows", 1)
            driven = total[:, : keep.shape[1]]
            mine = keep * mine + (1.0 - keep) * driven
            if RELAY and outer == 4 and piece % 16 == 0:
                up, down = outer_shift(mine, 1, inner), outer_shift(mine, -1, inner)
                h = piece // 2
                far = [outer_shift(up[:h], 1, inner), outer_shift(down[h:], -1, inner)]
                got = [mine, up] + far + [down]
            else:
                got = [mine] + [outer_shift(mine, k, inner) for k in range(1, outer)]
            state = jnp.concatenate(got, 0)
            if ride:
                blocks = lax.dynamic_slice_in_dim(total[:, keep.shape[1] :], y * tiles, tiles, 0)
            elif last:
                blocks = lax.psum_scatter(blocks, "rows", scatter_dimension=0, tiled=True)
        else:
            driven = lax.psum(driven, "rows")
            state = keep * state + (1.0 - keep) * driven
            if last:
                blocks = lax.psum_scatter(blocks, "rows", scatter_dimension=0, tiled=True)

    state = relative(state)
    ours, theirs = state[:, :states], swap(state[:, states:], "cols", 1)
    ours = ours.reshape(pairs, share, states)
    theirs = theirs.reshape(pairs, share, states)
    first = jnp.where(pair == 0, ours, theirs)
    second = jnp.where(pair == 0, theirs, ours)
    final = jnp.stack([first, second], 1).reshape(scen, states)
    blocks = jnp.transpose(blocks.reshape(tiles, STEPS, share), (1, 2, 0))
    return (final, temps, blocks)


def solution(mesh):
    placed = (
        P("rows", "cols"),
        P(None, "cols"),
        P("cols"),
        P("rows"),
        P("rows"),
        P(),
        P(None, None, "rows"),
    )
    return jax.shard_map(
        shards,
        mesh=mesh,
        in_specs=placed,
        out_specs=(P(None, "cols"), P("cols", "rows"), P(None, "cols", "rows")),
        check_vma=False,
    )
```
